128 devices in a mesh: row: 16 (over x, y_lo, core), col: 8 (over y_hi, z).
Axes of the slice: x: 4, y: 4 (y_hi: 2, y_lo: 2; y = y_hi * 2 + y_lo), z: 4, core: 2. Of those that a mesh axis runs over, the one named last changes fastest.
Arguments:
- vectors: bfloat16 [64, 1024, 512], P('col', 'row'), may hold values from -6 to 6
- right_factors: bfloat16 [64, 64, 1024, 128], P('row', 'col'), may hold values from -0.1875 to 0.1875
- left_factors: bfloat16 [64, 64, 1024, 128], P('row', 'col'), may hold values from -0.09375 to 0.09375
- tile_ranks: int32 [64, 64], P('row', 'col'), may hold values from 16 to 128
- owner_map: int32 [64], replicated, may hold values from 0 to 63, as said below
Outputs:
- applied: bfloat16 [64, 1024, 512], P('row', 'col')
The draws below stay inside these ranges and needn't reach their ends.
Inputs may be any that keep to these rules, and one draw needn't show every extreme that they name: owner_map is a permutation of 0 to 63; the 4 stored tile rows held by index i of row (stored rows i * 4 to i * 4 + 3) belong to 4 different indices of row of applied, i + c mod 16 for the same 4 offsets c at every i.
All inputs are finite; a program needn't handle non-finite values.
Results may differ from the reference program's by a relative error of at most 0.0066.
Values may be sent and summed in bfloat16 or wider, within the bound.
A program may use at most 128 MiB of HBM per device.

```python
import jax
import jax.numpy as jnp
from jax import lax

BLK = 1024
RMAX = 128
TRD = 4
NV = 512
NT = 64
MT = 64
N_ROW = 16


def shuffle(subkey):
    return jax.random.permutation(subkey, TRD)


def draw_owner_map(key, part):
    key_shift, key_dest, key_source = jax.random.split(jax.random.fold_in(key, 17), 3)
    offsets = jnp.arange(N_ROW, dtype=jnp.int32)
    ranking = jax.random.permutation(key_shift, N_ROW).astype(jnp.int32)
    priority = jnp.where(offsets == N_ROW // 2, -2, jnp.where(offsets == 1, -1, ranking))
    shifts = jnp.argsort(priority)[:TRD].astype(jnp.int32)
    dest_order = jax.vmap(shuffle)(jax.random.split(key_dest, N_ROW)).astype(jnp.int32)
    source_order = jax.vmap(shuffle)(jax.random.split(key_source, N_ROW)).astype(jnp.int32)
    source = jnp.arange(N_ROW, dtype=jnp.int32)[:, None]
    group_index = jnp.broadcast_to(jnp.arange(TRD, dtype=jnp.int32)[None, :], (N_ROW, TRD))
    target = (source + shifts[None, :]) % N_ROW
    landing = target * TRD + dest_order[target, group_index]
    places = source * TRD + source_order
    return jnp.zeros((MT,), jnp.int32).at[places.reshape(-1)].set(landing.reshape(-1))


def with_ends(entries, own_key, low, top_value):
    place = [jax.random.randint(jax.random.fold_in(own_key, axis), (), 0, length) for axis, length in enumerate(entries.shape)]
    main_axis = entries.shape.index(max(entries.shape))
    neighbour = place[:main_axis] + [(place[main_axis] + 1) % entries.shape[main_axis]] + place[main_axis + 1:]
    return entries.at[tuple(place)].set(low).at[tuple(neighbour)].set(top_value)


def block_scale(own_key, extent, cuts, least, largest):
    level, own = 1.0, jax.random.fold_in(own_key, 6)
    for axis_at, shards_of in cuts:
        heights = jnp.exp(jax.random.uniform(jax.random.fold_in(own, axis_at), (shards_of,), jnp.float32, least / len(cuts), largest / len(cuts)))
        level = level * jnp.repeat(heights, extent[axis_at] // shards_of).reshape([-1 if axis == axis_at else 1 for axis in range(len(extent))])
    return level


def centred(key, dims, width, limit, shards=(), kind=jnp.bfloat16):
    values = jax.random.normal(key, dims, jnp.float32) * width
    if len(shards) > 0:
        values = block_scale(key, dims, shards, -0.22, 0.18) * values
    return jnp.clip(values, min=-limit, max=limit).astype(kind)


def setup_inputs(seed: int = 0) -> dict:
    keys = jax.random.split(jax.random.key(seed), 6)
    return {
        "vectors": centred(keys[0], (NT, BLK, NV), 1.0, 6.0, ((0, 8), (1, 16))),
        "right_factors": centred(keys[1], (MT, NT, BLK, RMAX), BLK ** -0.5, 0.1875, ((0, 16), (1, 8))),
        "left_factors": centred(keys[2], (MT, NT, BLK, RMAX), (NT * RMAX // 2) ** -0.5, 0.09375, ((0, 16), (1, 8))),
        "tile_ranks": with_ends(jax.random.randint(keys[3], (MT, NT), RMAX // 8, RMAX + 1), jax.random.fold_in(keys[3], 1), RMAX // 8, RMAX).astype(jnp.int32),
        "owner_map": draw_owner_map(jax.random.fold_in(keys[5], 71), 0),
    }


def reference(vectors, right_factors, left_factors, tile_ranks, owner_map):
    columns = jnp.arange(RMAX, dtype=jnp.int32)
    wide_vectors = vectors.astype(jnp.float32)

    def tile_row(operands):
        left_row, right_row, rank_row = operands
        products = jnp.einsum("kbr,kbv->krv", right_row.astype(jnp.float32), wide_vectors)
        kept_mask = columns[None, :] < rank_row[:, None]
        coeffs = jnp.where(kept_mask[:, :, None], products, 0.0).astype(jnp.bfloat16)
        return jnp.einsum("kbr,krv->bv", left_row.astype(jnp.float32), coeffs.astype(jnp.float32))

    stored = lax.map(tile_row, (left_factors, right_factors, tile_ranks))
    natural = jnp.zeros(stored.shape, jnp.float32).at[owner_map].set(stored)
    return natural.astype(jnp.bfloat16)
```

```python
import functools

import jax
import jax.numpy as jnp
from jax import lax
from jax.experimental import pallas as pl
from jax.experimental.pallas import tpu as pltpu
from jax.sharding import PartitionSpec as P

MESH = pl.DeviceIdType.MESH
F32, BF16, I32 = jnp.float32, jnp.bfloat16, jnp.int32

NX, STEP_X, STEP_Y, STEP_CORE = 4, 4, 2, 1
NZ, NYH = 4, 2
CHUNKS = (256, 256)


def kernel(dims, *refs):
    held, ncol, blk, rank, share = dims
    nrow = blk // share
    ndst = NZ * NYH
    sub = blk // ndst
    piece = sub // nrow
    nt = len(CHUNKS)
    starts = [sum(CHUNKS[:t]) for t in range(nt)]
    refs = list(refs)
    vec, rf, lf, ranks, omap, out = refs[:6]
    raw, rt, lt, ssem, rsem, lsem, csem = refs[6:13]
    per = [refs[13 + 13 * t : 26 + 13 * t] for t in range(nt)]
    V, C, part, s1, s2, s3, s4, zown, fin, r1, send2, r2, _ = [list(a) for a in zip(*per)]

    i, d = lax.axis_index("row"), lax.axis_index("col")
    z, yh = lax.rem(d, NZ), lax.div(d, NZ)
    x = lax.div(i, STEP_X)
    inner = lax.rem(i, STEP_X)

    def at_x(dx):
        return lax.rem(x + dx + NX, NX) * STEP_X + inner

    def flip_y(r):
        return jnp.where(lax.rem(lax.div(r, STEP_Y), 2) == 0, r + STEP_Y, r - STEP_Y)

    def flip_core(r):
        return jnp.where(lax.rem(r, 2) == 0, r + 1, r - 1)

    def at_z(dz):
        return lax.rem(z + dz + NZ, NZ)

    iy, ic = flip_y(i), flip_core(i)
    xp, xm = at_x(1), at_x(-1)
    zp, zm, zo = at_z(1), at_z(-1), at_z(2)
    yo = 1 - yh

    loads = {}

    def load(name, src, dst):
        copy = pltpu.make_async_copy(src, dst, lsem.at[len(loads)])
        copy.start()
        loads[name] = copy

    def rows_of(t, j, k0=0, k1=ncol):
        return V[t].at[pl.ds(k0, k1 - k0), pl.ds(pl.multiple_of(j * share, share), share), :]

    for t in range(nt):
        load(("v", t), vec.at[:, :, pl.ds(starts[t], CHUNKS[t])], rows_of(t, i))
    for k in range(ncol):
        load(("r", k), rf.at[:, k], raw.at[:, k])
    load("l", lf, lt)

    bar = pltpu.get_barrier_semaphore()
    for m in range(1, nrow):
        pl.semaphore_signal(bar, 1, device_id={"row": lax.rem(i + m, nrow)}, device_id_type=MESH)
    for c in (yh * NZ + zp, yh * NZ + zm, yo * NZ + z):
        pl.semaphore_signal(bar, 1, device_id={"col": c}, device_id_type=MESH)
    pl.semaphore_wait(bar, nrow - 1 + 3)

    own = [omap[held * i + s] for s in range(held)]
    off = [lax.rem(lax.div(o, held) - i + nrow, nrow) for o in own]
    place = [sum((off[s] > off[u] if u > s else off[s] >= off[u]).astype(I32) for u in range(held) if u != s) for s in range(held)]
    sig = [sum(jnp.where(place[s] == q, s, 0) for s in range(held)) for q in range(held)]
    offq = [sum(jnp.where(place[s] == q, off[s], 0) for s in range(held)) for q in range(held)]
    lands = []
    for q in range(held):
        src = lax.rem(i - offq[q] + nrow, nrow)
        there = [omap[held * src + s] for s in range(held)]
        lands.append(sum(jnp.where(lax.div(o, held) == i, lax.rem(o, held), 0) for o in there))
    qof = [lax.rem(sum(jnp.where(lands[q] == o, q, 0) for q in range(held)), held) for o in range(held)]

    sent = {}

    def send(name, src, dst, dev):
        n = len(sent)
        copy = pltpu.make_async_remote_copy(
            src_ref=src, dst_ref=dst, send_sem=ssem.at[n], recv_sem=rsem.at[n], device_id=dev, device_id_type=MESH
        )
        copy.start()
        sent[name] = copy

    def got(*name):
        sent[name].wait_recv()

    def share_to(name, t, j, row, k0=0, k1=ncol):
        send(name, rows_of(t, j, k0, k1), rows_of(t, j, k0, k1), {"row": row})

    half = ncol // 2

    def a_own(t):
        loads["v", t].wait()
        share_to(("y", t), t, i, iy)
        share_to(("xp0", t), t, i, xp)
        share_to(("xm0", t), t, i, xm)
        share_to(("d0", t), t, i, ic)

    def a_part(t):
        got("y", t)
        share_to(("xp1", t), t, iy, xp)
        share_to(("xm1", t), t, iy, xm)
        share_to(("d1", t), t, iy, ic)

    def a_pass(t, n):
        lo, hi = (xm, xp) if n == 0 else (flip_y(xm), flip_y(xp))
        got(f"xp{n}", t)
        share_to((f"fp{n}", t), t, lo, xp, 0, half)
        share_to((f"dm{n}", t), t, lo, ic)
        got(f"xm{n}", t)
        share_to((f"fm{n}", t), t, hi, xm, half, ncol)
        share_to((f"dp{n}", t), t, hi, ic)

    def a_last(t, n):
        far = at_x(2) if n == 0 else flip_y(at_x(2))
        got(f"fp{n}", t)
        share_to((f"df{n}", t), t, far, ic, 0, half)
        got(f"fm{n}", t)
        share_to((f"dg{n}", t), t, far, ic, half, ncol)

    def a_end(t):
        for n in range(2):
            for name in ("d", "dm", "dp", "df", "dg"):
                got(f"{name}{n}", t)

    def turn(k0, k1):
        for k in range(k0, k1):
            loads["r", k].wait()

        def one(n, carry):
            k, s = k0 + lax.div(n, held), lax.rem(n, held)
            rt[k, pl.ds(pl.multiple_of(s * rank, rank), rank), :] = raw[s, k].T
            return carry

        lax.fori_loop(0, (k1 - k0) * held, one, 0)

    def m1(t):
        width = CHUNKS[t]

        def one(k, carry):
            acc = jnp.dot(rt[k], V[t][k], preferred_element_type=F32)
            for s in range(held):
                kept = lax.broadcasted_iota(I32, (rank, width), 0) < ranks[s, k]
                C[t][s, pl.ds(pl.multiple_of(k * rank, rank), rank), :] = jnp.where(
                    kept, acc[s * rank : (s + 1) * rank], 0.0
                ).astype(BF16)
            return carry

        lax.fori_loop(0, ncol, one, 0)

    def m2(t, q, blocks):
        slot = sig[q]
        left = [
            jnp.concatenate(
                [lt[slot, k, pl.ds(pl.multiple_of((y * NZ + w) * sub, sub), sub), :] for k in range(ncol)], axis=1
            )
            for y, w in blocks
        ]
        res = jnp.dot(jnp.concatenate(left, axis=0), C[t][slot], preferred_element_type=F32).astype(BF16)
        for n, (y, w) in enumerate(blocks):
            part[t][q, y, w] = res[n * sub : (n + 1) * sub]

    def col_z(w):
        return {"col": yh * NZ + w}

    def b_first(t, q):
        m2(t, q, [(0, zo), (1, zo), (1, zp), (0, zm)])
        send(("s1p", t, q), part[t].at[q, 0, zo], s1[t].at[q, 0], col_z(zp))
        send(("s1m", t, q), part[t].at[q, 1, zo], s1[t].at[q, 1], col_z(zm))
        send(("s2p", t, q), part[t].at[q, 1, zp], s2[t].at[q, 0], col_z(zp))
        send(("s2m", t, q), part[t].at[q, 0, zm], s2[t].at[q, 1], col_z(zm))
        m2(t, q, [(0, zp), (1, zm), (0, z), (1, z)])

    def b_pass(t, q):
        got("s1p", t, q)
        part[t][q, 0, zp] = (part[t][q, 0, zp].astype(F32) + s1[t][q, 0].astype(F32)).astype(BF16)
        send(("s3p", t, q), part[t].at[q, 0, zp], s3[t].at[q, 0], col_z(zp))
        got("s1m", t, q)
        part[t][q, 1, zm] = (part[t][q, 1, zm].astype(F32) + s1[t][q, 1].astype(F32)).astype(BF16)
        send(("s3m", t, q), part[t].at[q, 1, zm], s3[t].at[q, 1], col_z(zm))

    def b_sum(t, q):
        got("s2p", t, q)
        got("s2m", t, q)
        got("s3p", t, q)
        got("s3m", t, q)
        low = part[t][q, 0, z].astype(F32) + (s3[t][q, 0].astype(F32) + s2[t][q, 1].astype(F32))
        high = part[t][q, 1, z].astype(F32) + (s2[t][q, 0].astype(F32) + s3[t][q, 1].astype(F32))
        here = yh == 0
        zown[t][q] = jnp.where(here, low, high)
        part[t][q, 0, z] = jnp.where(here, high, low).astype(BF16)
        send(("s4", t, q), part[t].at[q, 0, z], s4[t].at[q], {"col": yo * NZ + z})

    def b_end(t, q):
        got("s4", t, q)
        total = (zown[t][q] + s4[t][q].astype(F32)).reshape(nrow, piece, CHUNKS[t]).astype(BF16)
        fin[t][:, q] = total
        r1[t][0, q] = total[0]

    def spread(t, phase, src, dst):
        for m in range(1, nrow):
            pltpu.make_async_remote_copy(
                src_ref=src.at[m],
                dst_ref=dst.at[m],
                send_sem=csem.at[t, phase, 0],
                recv_sem=csem.at[t, phase, 1],
                device_id={"row": lax.rem(i + m, nrow)},
                device_id_type=MESH,
            ).start()

    def spread_all(t, phase, src, dst):
        return pltpu.make_async_remote_copy(
            src_ref=src.at[pl.ds(1, nrow - 1)],
            dst_ref=dst.at[pl.ds(1, nrow - 1)],
            send_sem=csem.at[t, phase, 0],
            recv_sem=csem.at[t, phase, 1],
            device_id={"row": lax.rem(i + 1, nrow)},
            device_id_type=MESH,
        )

    def c_first(t):
        spread(t, 0, fin[t], r1[t])

    def c_second(t):
        spread_all(t, 0, fin[t], r1[t]).wait_recv()
        for q in range(held):
            r2[t][0, q] = r1[t][offq[q], q]
            for e in range(1, nrow):
                send2[t][e, q] = r1[t][lax.rem(offq[q] - e + nrow, nrow), q]
        spread(t, 1, send2[t], r2[t])

    def c_end(t):
        spread_all(t, 1, send2[t], r2[t]).wait_recv()
        for o in range(held):
            q = qof[o]
            shift = sum(jnp.where(q == u, offq[u], 0) for u in range(held))
            for m in range(nrow):
                out[o, m, :, starts[t] : starts[t] + CHUNKS[t]] = r2[t][lax.rem(shift - m + nrow, nrow), q]

    for t in range(nt):
        a_own(t)
    turn(0, ncol // 2)
    a_part(0)
    a_pass(0, 0)
    turn(ncol // 2, ncol)
    a_pass(0, 1)
    loads["l"].wait()
    a_part(1)
    a_pass(1, 0)
    a_last(0, 0)
    a_last(0, 1)
    a_end(0)
    m1(0)
    a_pass(1, 1)
    b_first(0, 0)
    a_last(1, 0)
    b_first(0, 1)
    b_pass(0, 0)
    a_last(1, 1)
    b_first(0, 2)
    b_pass(0, 1)
    b_sum(0, 0)
    a_end(1)
    b_first(0, 3)
    b_pass(0, 2)
    b_sum(0, 1)
    m1(1)
    b_pass(0, 3)
    b_sum(0, 2)
    b_end(0, 0)
    b_first(1, 0)
    b_sum(0, 3)
    b_end(0, 1)
    b_first(1, 1)
    b_pass(1, 0)
    b_end(0, 2)
    b_first(1, 2)
    b_pass(1, 1)
    b_sum(1, 0)
    b_end(0, 3)
    c_first(0)
    b_first(1, 3)
    b_pass(1, 2)
    b_sum(1, 1)
    b_end(1, 0)
    c_second(0)
    b_pass(1, 3)
    b_sum(1, 2)
    b_end(1, 1)
    c_end(0)
    b_sum(1, 3)
    b_end(1, 2)
    b_end(1, 3)
    c_first(1)
    c_second(1)
    c_end(1)

    for copy in sent.values():
        copy.wait_send()
    for t in range(nt):
        spread_all(t, 0, fin[t], r1[t]).wait_send()
        spread_all(t, 1, send2[t], r2[t]).wait_send()


def on_device(vectors, right_factors, left_factors, tile_ranks, owner_map):
    held, ncol, blk, rank = right_factors.shape
    share, nvec = vectors.shape[1:]
    nrow, ndst = lax.axis_size("row"), lax.axis_size("col")
    sub = blk // ndst
    piece = sub // nrow
    nsend = len(CHUNKS) * (19 + 7 * held)
    scratch = [
        pltpu.VMEM((held, ncol, blk, rank), BF16),
        pltpu.VMEM((ncol, held * rank, blk), BF16),
        pltpu.VMEM((held, ncol, blk, rank), BF16),
        pltpu.SemaphoreType.DMA((nsend,)),
        pltpu.SemaphoreType.DMA((nsend,)),
        pltpu.SemaphoreType.DMA((len(CHUNKS) + ncol + 1,)),
        pltpu.SemaphoreType.DMA((len(CHUNKS), 2, 2)),
    ]
    for w in CHUNKS:
        scratch += [
            pltpu.VMEM((ncol, blk, w), BF16),
            pltpu.VMEM((held, ncol * rank, w), BF16),
            pltpu.VMEM((held, NYH, NZ, sub, w), BF16),
            pltpu.VMEM((held, 2, sub, w), BF16),
            pltpu.VMEM((held, 2, sub, w), BF16),
            pltpu.VMEM((held, 2, sub, w), BF16),
            pltpu.VMEM((held, sub, w), BF16),
            pltpu.VMEM((held, sub, w), F32),
            pltpu.VMEM((nrow, held, piece, w), BF16),
            pltpu.VMEM((nrow, held, piece, w), BF16),
            pltpu.VMEM((nrow, held, piece, w), BF16),
            pltpu.VMEM((nrow, held, piece, w), BF16),
            pltpu.SMEM((1,), I32),
        ]
    hbm = pl.BlockSpec(memory_space=pl.ANY)
    smem = pl.BlockSpec(memory_space=pltpu.SMEM)
    applied = pl.pallas_call(
        functools.partial(kernel, (held, ncol, blk, rank, share)),
        out_shape=jax.ShapeDtypeStruct((held, nrow, piece, nvec), BF16),
        in_specs=[hbm, hbm, hbm, smem, smem],
        out_specs=pl.BlockSpec(memory_space=pltpu.VMEM),
        scratch_shapes=scratch,
        compiler_params=pltpu.CompilerParams(
            collective_id=0, has_side_effects=True, vmem_limit_bytes=62 * 2**20
        ),
    )(vectors, right_factors, left_factors, tile_ranks, owner_map)
    return applied.reshape(held, sub, nvec)


def solution(mesh):
    placed = (
        P("col", "row", None),
        P("row", "col", None, None),
        P("row", "col", None, None),
        P("row", "col"),
        P(),
    )
    return jax.shard_map(
        on_device, mesh=mesh, in_specs=placed, out_specs=P("row", "col", None), check_vma=False
    )
```
